256 devices in a mesh: dp: 32 (over z, x_lo, core), tp: 8 (over y, x_hi).
Axes of the slice: x: 4 (x_hi: 2, x_lo: 2; x = x_hi * 2 + x_lo), y: 4, z: 8, core: 2. Of those that a mesh axis runs over, the one named last changes fastest.
Arguments:
- gate_pre: bfloat16 [24576, 7168], P('dp', 'tp'), may hold values from -6 to 6
- up_pre: bfloat16 [24576, 7168], P('dp', 'tp'), may hold values from -6 to 6
- target: bfloat16 [24576, 2048], P('dp', 'tp'), may hold values from -6 to 6
- norm_gain: float32 [2048], P('tp'), may hold values from 0.5 to 1.5
- weight: bfloat16 [32, 7168, 2048], P('dp', 'tp'), may hold values from -6 to 6
- round_index: int32 [1], replicated, may hold values from 0 to 9999
Outputs:
- normed: bfloat16 [24576, 2048], P('dp', 'tp')
- mixed: bfloat16 [32, 7168, 2048], P('dp', 'tp')
The draws below stay inside these ranges and needn't reach their ends.
All inputs are finite; a program needn't handle non-finite values.
Results may differ from the reference program's by a relative error of at most 0.001.
The reference program's roundings to bfloat16 on the way (of `hidden`, `grad_out` and `updated`) count: a program that leaves them out, or rounds other values in their place, can miss the bound.
Values may be sent and summed in bfloat16 or wider, within the bound.
No kernel may reach another device: no remote copies, remote signals or barrier semaphores. Data moves between devices by JAX's collectives and lax.ppermute only.
A program may use at most 64 MiB of HBM per device.

```python
import math
import jax
import jax.numpy as jnp
from jax import lax

D = 2048
FF = 7168
TOK = 768
TOKENS = 24576
N_DP = 32


def block_scale(key, dims, pieces, smallest, high):
    factor_of, own = 1.0, jax.random.fold_in(key, 6)
    for dim, shards_of in pieces:
        steps = jnp.exp(jax.random.uniform(jax.random.fold_in(own, dim), (shards_of,), jnp.float32, smallest / len(pieces), high / len(pieces)))
        factor_of = factor_of * jnp.repeat(steps, dims[dim] // shards_of).reshape([-1 if axis == dim else 1 for axis in range(len(dims))])
    return factor_of


def centred(key, extent, scale, reach, split=(), kind=jnp.bfloat16):
    drawn = jax.random.normal(key, extent, jnp.float32) * scale
    if len(split) > 0:
        drawn = block_scale(key, extent, split, -0.22, 0.18) * drawn
    return jnp.clip(drawn, min=-reach, max=reach).astype(kind)


def setup_inputs(seed: int = 0) -> dict:
    arg_keys = jax.random.split(jax.random.key(seed), 7)
    gate_pre = centred(arg_keys[0], (TOKENS, FF), 1.0, 6.0, ((0, 32), (1, 8)))
    up_pre = centred(arg_keys[1], (TOKENS, FF), 1.0, 6.0, ((0, 32), (1, 8)))
    target = centred(arg_keys[2], (TOKENS, D), 1.0, 6.0, ((0, 32), (1, 8)))
    norm_gain = jnp.clip(1.0 + 0.1 * jax.random.normal(arg_keys[3], (D,), jnp.float32), 0.5, 1.5)
    weight = centred(arg_keys[4], (N_DP, FF, D), 1.0, 6.0, ((0, 32), (1, 8)))
    round_index = jax.random.randint(arg_keys[5], (1,), 0, 10000).astype(jnp.int32)
    return {"gate_pre": gate_pre, "up_pre": up_pre, "target": target, "norm_gain": norm_gain, "weight": weight, "round_index": round_index}


EPSILON = 1e-06

def step_rate(round_index):
    phase = (round_index[0] % 1000).astype(jnp.float32) * jnp.float32(2.0 * math.pi / 1000.0)
    return jnp.float32(0.25) * (jnp.float32(0.55) + jnp.float32(0.45) * jnp.cos(phase))

def replica_step(inputs, norm_gain, rate):
    gate_rows, up_rows, target_rows, weight_rows = inputs
    out_scale = FF ** (-0.5)
    hidden = (jax.nn.silu(gate_rows.astype(jnp.float32)) * up_rows.astype(jnp.float32)).astype(jnp.bfloat16)
    summed = jnp.dot(hidden, weight_rows, preferred_element_type=jnp.float32) * out_scale
    inv_rms = lax.rsqrt(lax.optimization_barrier(jnp.mean(summed * summed, axis=1, keepdims=True)) + EPSILON)
    normal = summed * inv_rms
    output = normal * norm_gain
    grad_norm = (output - target_rows.astype(jnp.float32)) * norm_gain
    inner = lax.optimization_barrier(jnp.mean(grad_norm * normal, axis=1, keepdims=True))
    grad_out = (inv_rms * (grad_norm - normal * inner)).astype(jnp.bfloat16)
    weight_grad = lax.dot_general(hidden, grad_out, (((0,), (0,)), ((), ())), preferred_element_type=jnp.float32) * out_scale
    updated = (weight_rows.astype(jnp.float32) - rate * weight_grad).astype(jnp.bfloat16)
    return (output.astype(jnp.bfloat16), updated)

def reference(gate_pre, up_pre, target, norm_gain, weight, round_index):
    gate_blocks = gate_pre.reshape(N_DP, TOK, FF)
    up_blocks = up_pre.reshape(N_DP, TOK, FF)
    target_blocks = target.reshape(N_DP, TOK, D)
    rate = step_rate(round_index)

    def one_replica(inputs):
        return replica_step(inputs, norm_gain, rate)
    normed, updated = lax.map(one_replica, (gate_blocks, up_blocks, target_blocks, weight))
    levels = N_DP.bit_length() - 1
    offset = jnp.left_shift(jnp.int32(1), (round_index[0] % levels).astype(jnp.int32))
    source = ((jnp.arange(N_DP, dtype=jnp.int32) - offset) % N_DP).astype(jnp.int32)
    peer_rows = updated[source]
    mixed = (0.5 * (updated.astype(jnp.float32) + peer_rows.astype(jnp.float32))).astype(jnp.bfloat16)
    return (normed.reshape(N_DP * TOK, D), mixed)
```

```python
import functools
import math

import jax
import jax.numpy as jnp
from jax import lax
from jax.experimental import pallas as pl
from jax.experimental.pallas import tpu as pltpu
from jax.sharding import Mesh
from jax.sharding import PartitionSpec as P

FF = 7168
D = 2048
EPSILON = 1e-06
TP = ("tp_0", "tp_1")
BLOCK = 128
CODES = 16
F32, BF16 = jnp.float32, jnp.bfloat16

EARLY = (0, 0, 512, 384, 384)


def step_rate(round_index):
    phase = (round_index[0] % 1000).astype(F32) * jnp.float32(2.0 * math.pi / 1000.0)
    return jnp.float32(0.25) * (jnp.float32(0.55) + jnp.float32(0.45) * jnp.cos(phase))


def columns_of(rows):
    filled = jnp.concatenate([rows, jnp.zeros((BLOCK - rows.shape[0], BLOCK), F32)], axis=0)
    return filled.T


def forward_kernel(gate_ref, up_ref, weight_ref, hidden_t_ref, coded_ref, scale_scr):
    step = pl.program_id(0)
    hidden = jax.nn.silu(gate_ref[...].astype(F32)) * up_ref[...].astype(F32)
    hidden_t_ref[...] = hidden.T.astype(BF16)
    partial = jnp.dot(hidden.astype(BF16), weight_ref[...], preferred_element_type=F32) * FF ** (-0.5)
    top = jnp.max(jnp.abs(partial), axis=1, keepdims=True)
    level = jnp.ceil(8.0 * jnp.log2(jnp.maximum(top, 1e-30))) + 1.0
    scaled = partial * jnp.exp2(15.0 - 0.125 * level)
    width = coded_ref.shape[2]
    rows = pl.ds(pl.multiple_of(step * BLOCK, BLOCK), BLOCK)
    for part in range(coded_ref.shape[0]):
        values = scaled[:, part * width : (part + 1) * width]
        coded_ref[part, rows, :] = jnp.round(values).astype(jnp.int32).astype(jnp.int16)
    scale_scr[pl.ds(step, 1), :] = jnp.broadcast_to(level, (BLOCK, BLOCK)).T[:1, :]

    @pl.when(step == pl.num_programs(0) - 1)
    def _():
        codes = scale_scr[...].astype(jnp.int32).astype(jnp.int16)
        tokens = coded_ref.shape[1] - CODES
        for part in range(coded_ref.shape[0]):
            coded_ref[part, tokens:, :BLOCK] = codes
            coded_ref[part, tokens:, BLOCK:] = codes


def forward(gate, up, weight, parts):
    tokens, units = gate.shape
    width = weight.shape[1] // parts
    return pl.pallas_call(
        forward_kernel,
        grid=(tokens // BLOCK,),
        in_specs=[
            pl.BlockSpec((BLOCK, units), lambda i: (i, 0)),
            pl.BlockSpec((BLOCK, units), lambda i: (i, 0)),
            pl.BlockSpec(weight.shape, lambda i: (0, 0)),
        ],
        out_specs=[
            pl.BlockSpec((units, BLOCK), lambda i: (0, i)),
            pl.BlockSpec((parts, tokens + CODES, width), lambda i: (0, 0, 0)),
        ],
        out_shape=[
            jax.ShapeDtypeStruct((units, tokens), BF16),
            jax.ShapeDtypeStruct((parts, tokens + CODES, width), jnp.int16),
        ],
        scratch_shapes=[pltpu.VMEM((CODES, BLOCK), F32)],
        name="forward",
    )(gate, up, weight)


def share_kernel(coded_ref, codes_ref, target_ref, gain_ref, share_ref, stats_ref):
    step = pl.program_id(0)
    parts = coded_ref.shape[0]
    codes = codes_ref[...][:, :, :BLOCK].astype(jnp.int32).astype(F32)
    here = lax.broadcasted_iota(jnp.int32, codes.shape, 1) == step
    levels = columns_of(jnp.sum(jnp.where(here, codes, 0.0), axis=1))
    share = jnp.zeros(share_ref.shape, F32)
    for part in range(parts):
        factor = jnp.exp2(0.125 * levels[:, part : part + 1] - 15.0)
        share += coded_ref[part].astype(jnp.int32).astype(F32) * factor
    share_ref[...] = share
    gain = gain_ref[...]
    scaled = share * gain
    square = jnp.sum(share * share, axis=1, keepdims=True)
    gained = jnp.sum(scaled * scaled, axis=1, keepdims=True)
    crossed = jnp.sum(target_ref[...].astype(F32) * scaled, axis=1, keepdims=True)
    lane = lax.broadcasted_iota(jnp.int32, (BLOCK, BLOCK), 1)
    packed = jnp.where(lane == 0, square, jnp.where(lane == 1, gained, jnp.where(lane == 2, crossed, 0.0)))
    stats_ref[...] = packed.T[:8, :]


def share_and_stats(coded, target, gain):
    parts, rows, width = coded.shape
    tokens = target.shape[0]
    return pl.pallas_call(
        share_kernel,
        grid=(tokens // BLOCK,),
        in_specs=[
            pl.BlockSpec((parts, BLOCK, width), lambda i: (0, i, 0)),
            pl.BlockSpec((parts, CODES, width), lambda i: (0, tokens // CODES, 0)),
            pl.BlockSpec((BLOCK, width), lambda i: (i, 0)),
            pl.BlockSpec((1, width), lambda i: (0, 0)),
        ],
        out_specs=[
            pl.BlockSpec((BLOCK, width), lambda i: (i, 0)),
            pl.BlockSpec((8, BLOCK), lambda i: (0, i)),
        ],
        out_shape=[
            jax.ShapeDtypeStruct((tokens, width), F32),
            jax.ShapeDtypeStruct((8, tokens), F32),
        ],
        name="share",
    )(coded, coded, target, gain)


def grad_kernel(share_ref, stats_ref, target_ref, gain_ref, normed_ref, grad_ref, copies_ref):
    stats = jnp.sum(stats_ref[...], axis=0)
    features = share_ref.shape[1] * stats_ref.shape[0]
    square, gained, crossed = stats[0:1, :], stats[1:2, :], stats[2:3, :]
    inv_rms = lax.rsqrt(square / features + EPSILON)
    inner = inv_rms * (inv_rms * gained - crossed) / features
    columns = columns_of(jnp.concatenate([inv_rms, inner, jnp.zeros((6, BLOCK), F32)], axis=0))
    inv_col, inner_col = columns[:, 0:1], columns[:, 1:2]
    gain = gain_ref[...]
    normal = share_ref[...] * inv_col
    output = normal * gain
    grad_norm = (output - target_ref[...].astype(F32)) * gain
    grad = (inv_col * (grad_norm - normal * inner_col)).astype(BF16)
    normed_ref[...] = output.astype(BF16)
    grad_ref[...] = grad
    for part in range(copies_ref.shape[0]):
        copies_ref[part] = grad


def grads(share, stats, target, gain):
    tokens, width = share.shape
    parts = stats.shape[0]
    block = pl.BlockSpec((BLOCK, width), lambda i: (i, 0))
    return pl.pallas_call(
        grad_kernel,
        grid=(tokens // BLOCK,),
        in_specs=[
            block,
            pl.BlockSpec((parts, 8, BLOCK), lambda i: (0, 0, i)),
            block,
            pl.BlockSpec((1, width), lambda i: (0, 0)),
        ],
        out_specs=[block, block, pl.BlockSpec((parts, BLOCK, width), lambda i: (0, i, 0))],
        out_shape=[
            jax.ShapeDtypeStruct((tokens, width), BF16),
            jax.ShapeDtypeStruct((tokens, width), BF16),
            jax.ShapeDtypeStruct((parts, tokens, width), BF16),
        ],
        name="grads",
    )(share, stats, target, gain)


def updated_block(rate_ref, hidden_ref, grad_ref, weight_ref, part):
    width = grad_ref.shape[2]
    weight_grad = jnp.dot(hidden_ref[...], grad_ref[part], preferred_element_type=F32) * FF ** (-0.5)
    columns = slice(part * width, (part + 1) * width)
    return (weight_ref[:, columns].astype(F32) - rate_ref[0] * weight_grad).astype(BF16), columns


def update_kernel(rate_ref, hidden_ref, grad_ref, weight_ref, updated_ref):
    for part in range(grad_ref.shape[0]):
        updated, columns = updated_block(rate_ref, hidden_ref, grad_ref, weight_ref, part)
        updated_ref[:, columns] = updated


def update(rate, hidden_t, grad, weight, first, last):
    tokens, features = hidden_t.shape[1], weight.shape[1]
    skip = first // BLOCK
    return pl.pallas_call(
        update_kernel,
        grid=((last - first) // BLOCK,),
        in_specs=[
            pl.BlockSpec(memory_space=pltpu.SMEM),
            pl.BlockSpec((BLOCK, tokens), lambda i: (i + skip, 0)),
            pl.BlockSpec(grad.shape, lambda i: (0, 0, 0)),
            pl.BlockSpec((BLOCK, features), lambda i: (i + skip, 0)),
        ],
        out_specs=pl.BlockSpec((BLOCK, features), lambda i: (i, 0)),
        out_shape=jax.ShapeDtypeStruct((last - first, features), BF16),
        name="update",
    )(rate, hidden_t, grad, weight)


def averaged(one, other):
    return (0.5 * (one.astype(F32) + other.astype(F32))).astype(BF16)


def mix_early_kernel(rate_ref, hidden_ref, grad_ref, weight_ref, own_ref, mixed_ref):
    for part in range(grad_ref.shape[0]):
        peer, columns = updated_block(rate_ref, hidden_ref, grad_ref, weight_ref, part)
        mixed_ref[:, columns] = averaged(own_ref[:, columns], peer)


def mix_early(rate, hidden_t, grad, weight, own, rows):
    early, tokens = hidden_t.shape
    features = weight.shape[1]
    block = pl.BlockSpec((BLOCK, features), lambda i: (i, 0))
    return pl.pallas_call(
        mix_early_kernel,
        grid=(early // BLOCK,),
        in_specs=[
            pl.BlockSpec(memory_space=pltpu.SMEM),
            pl.BlockSpec((BLOCK, tokens), lambda i: (i, 0)),
            pl.BlockSpec(grad.shape, lambda i: (0, 0, 0)),
            block,
            block,
        ],
        out_specs=block,
        out_shape=jax.ShapeDtypeStruct((rows, features), BF16),
        name="mix_early",
    )(rate, hidden_t, grad, weight, own)


def mix_late_kernel(own_ref, peer_ref, held_ref, mixed_ref):
    mixed_ref[...] = averaged(own_ref[...], peer_ref[...])


def mix_late(own, peer, held):
    late, features = own.shape
    skip = (held.shape[0] - late) // BLOCK
    block = pl.BlockSpec((BLOCK, features), lambda i: (i, 0))
    return pl.pallas_call(
        mix_late_kernel,
        grid=(late // BLOCK,),
        in_specs=[block, block, pl.BlockSpec(memory_space=pl.ANY)],
        out_specs=pl.BlockSpec((BLOCK, features), lambda i: (i + skip, 0)),
        out_shape=jax.ShapeDtypeStruct(held.shape, BF16),
        input_output_aliases={2: 0},
        name="mix_late",
    )(own, peer, held)


def exchanged(parts):
    return lax.all_to_all(parts, TP, split_axis=0, concat_axis=0, tiled=True)


def step(level, gate, up, target, gain, weight, rate):
    count = lax.axis_size("dp")
    parts = lax.axis_size(TP)
    rows = weight.shape[0]
    early = EARLY[level]

    def to_peer(array):
        by = 1 << level
        return lax.ppermute(array, "dp", [(i, (i + by) % count) for i in range(count)])

    if early:
        peer_weight = to_peer(weight[:early])
    hidden_t, coded = forward(gate, up, weight, parts)
    if early:
        peer_hidden = to_peer(hidden_t[:early])
    share, stats = share_and_stats(exchanged(coded), target, gain)
    stats = exchanged(jnp.broadcast_to(stats, (parts, *stats.shape)))
    normed, grad_share, copies = grads(share, stats, target, gain)
    if early:
        peer_share = to_peer(grad_share)
    grad = exchanged(copies)
    own_late = update(rate, hidden_t, grad, weight, early, rows)
    peer_late = to_peer(own_late)
    if not early:
        return normed, averaged(own_late, peer_late)
    peer_grad = exchanged(jnp.broadcast_to(peer_share, (parts, *peer_share.shape)))
    own_early = update(rate, hidden_t, grad, weight, 0, early)
    held = mix_early(rate, peer_hidden, peer_grad, peer_weight, own_early, rows)
    return normed, mix_late(own_late, peer_late, held)


def shards(gate_pre, up_pre, target, norm_gain, weight, round_index):
    rate = step_rate(round_index).reshape(1)
    levels = lax.axis_size("dp").bit_length() - 1
    level = round_index[0] % levels
    branches = [functools.partial(step, number) for number in range(levels)]
    normed, mixed = lax.switch(level, branches, gate_pre, up_pre, target, norm_gain[None], weight[0], rate)
    return normed, mixed[None]


def solution(mesh):
    finer = Mesh(mesh.devices.reshape(mesh.shape["dp"], 4, 2), ("dp", "tp_0", "tp_1"))
    placed = (P("dp", TP), P("dp", TP), P("dp", TP), P(TP), P("dp", TP, None), P())
    return jax.shard_map(
        shards,
        mesh=finer,
        in_specs=placed,
        out_specs=(P("dp", TP), P("dp", TP, None)),
        check_vma=False,
    )
```

```python
import functools
import math

import jax
import jax.numpy as jnp
from jax import lax
from jax.experimental import pallas as pl
from jax.experimental.pallas import tpu as pltpu
from jax.sharding import Mesh
from jax.sharding import PartitionSpec as P


FF = 7168
EPSILON = 1e-06
TP = ("tp_0", "tp_1")
BLOCK = 128
CODES = 16
F32, BF16 = jnp.float32, jnp.bfloat16

PLANS = (
    (0, 0, 224, True, True, False),
    (0, 0, 224, True, True, False),
    (0, 672, 224, False, False, True),
    (224, 336, 112, False, False, False),
    (0, 448, 224, True, False, False),
)


def step_rate(round_index):
    phase = (round_index[0] % 1000).astype(F32) * jnp.float32(2.0 * math.pi / 1000.0)
    return jnp.float32(0.25) * (jnp.float32(0.55) + jnp.float32(0.45) * jnp.cos(phase))


def columns_of(rows):
    filled = jnp.concatenate([rows, jnp.zeros((BLOCK - rows.shape[0], BLOCK), F32)], axis=0)
    return filled.T


def columns_at(number, width):
    return pl.ds(pl.multiple_of(number * width, width), width)


def forward_kernel(gate_ref, up_ref, weight_ref, hidden_t_ref, coded_ref, scale_scr, partial_scr):
    step = pl.program_id(0)
    hidden = jax.nn.silu(gate_ref[...].astype(F32)) * up_ref[...].astype(F32)
    hidden_t_ref[...] = hidden.T.astype(BF16)
    hidden = hidden.astype(BF16)
    parts, _, width = coded_ref.shape

    def products(number, top):
        weight = weight_ref[:, columns_at(number, 4 * width)]
        partial = jnp.dot(hidden, weight, preferred_element_type=F32) * FF ** (-0.5)
        for part in range(4):
            values = partial[:, part * width : (part + 1) * width]
            partial_scr[4 * number + part] = values
            for lanes in range(0, width, BLOCK):
                top = jnp.maximum(top, jnp.abs(values[:, lanes : lanes + BLOCK]))
        return top

    top = lax.fori_loop(0, parts // 4, products, jnp.zeros((BLOCK, BLOCK), F32))
    top = jnp.max(top, axis=1, keepdims=True)
    level = jnp.ceil(8.0 * jnp.log2(jnp.maximum(top, 1e-30))) + 1.0
    factor = jnp.exp2(15.0 - 0.125 * level)
    rows = pl.ds(pl.multiple_of(step * BLOCK, BLOCK), BLOCK)

    def coding(part, _):
        coded_ref[part, rows, :] = jnp.round(partial_scr[part] * factor).astype(jnp.int32).astype(jnp.int16)
        return 0

    lax.fori_loop(0, parts, coding, 0)
    scale_scr[pl.ds(step, 1), :] = jnp.broadcast_to(level, (BLOCK, BLOCK)).T[:1, :]

    @pl.when(step == pl.num_programs(0) - 1)
    def _():
        codes = scale_scr[...].astype(jnp.int32).astype(jnp.int16)
        tokens = coded_ref.shape[1] - CODES
        for part in range(parts):
            coded_ref[part, tokens:, :BLOCK] = codes
            coded_ref[part, tokens:, BLOCK:] = codes


def forward(gate, up, weight, parts):
    tokens, units = gate.shape
    width = weight.shape[1] // parts
    return pl.pallas_call(
        forward_kernel,
        grid=(tokens // BLOCK,),
        in_specs=[
            pl.BlockSpec((BLOCK, units), lambda i: (i, 0)),
            pl.BlockSpec((BLOCK, units), lambda i: (i, 0)),
            pl.BlockSpec(weight.shape, lambda i: (0, 0)),
        ],
        out_specs=[
            pl.BlockSpec((units, BLOCK), lambda i: (0, i)),
            pl.BlockSpec((parts, tokens + CODES, width), lambda i: (0, 0, 0)),
        ],
        out_shape=[
            jax.ShapeDtypeStruct((units, tokens), BF16),
            jax.ShapeDtypeStruct((parts, tokens + CODES, width), jnp.int16),
        ],
        scratch_shapes=[pltpu.VMEM((CODES, BLOCK), F32), pltpu.VMEM((parts, BLOCK, width), F32)],
        name="forward",
    )(gate, up, weight)


def share_kernel(coded_ref, codes_ref, target_ref, gain_ref, share_ref, stats_ref):
    step = pl.program_id(0)
    parts = coded_ref.shape[0]
    codes = codes_ref[...][:, :, :BLOCK].astype(jnp.int32).astype(F32)
    here = lax.broadcasted_iota(jnp.int32, codes.shape, 1) == step
    factors = columns_of(jnp.exp2(0.125 * jnp.sum(jnp.where(here, codes, 0.0), axis=1) - 15.0))
    share = jnp.zeros(share_ref.shape, F32)
    for part in range(parts):
        share += coded_ref[part].astype(jnp.int32).astype(F32) * factors[:, part : part + 1]
    share_ref[...] = share
    gain = gain_ref[...]
    scaled = share * gain
    square = jnp.sum(share * share, axis=1, keepdims=True)
    gained = jnp.sum(scaled * scaled, axis=1, keepdims=True)
    crossed = jnp.sum(target_ref[...].astype(F32) * scaled, axis=1, keepdims=True)
    lane = lax.broadcasted_iota(jnp.int32, (BLOCK, BLOCK), 1)
    packed = jnp.where(lane == 0, square, jnp.where(lane == 1, gained, jnp.where(lane == 2, crossed, 0.0)))
    stats = packed.T[:8, :]
    for part in range(parts):
        stats_ref[part] = stats


def share_and_stats(coded, target, gain):
    parts, _, width = coded.shape
    tokens = target.shape[0]
    return pl.pallas_call(
        share_kernel,
        grid=(tokens // BLOCK,),
        in_specs=[
            pl.BlockSpec((parts, BLOCK, width), lambda i: (0, i, 0)),
            pl.BlockSpec((parts, CODES, width), lambda i: (0, tokens // CODES, 0)),
            pl.BlockSpec((BLOCK, width), lambda i: (i, 0)),
            pl.BlockSpec((1, width), lambda i: (0, 0)),
        ],
        out_specs=[
            pl.BlockSpec((BLOCK, width), lambda i: (i, 0)),
            pl.BlockSpec((parts, 8, BLOCK), lambda i: (0, 0, i)),
        ],
        out_shape=[
            jax.ShapeDtypeStruct((tokens, width), F32),
            jax.ShapeDtypeStruct((parts, 8, tokens), F32),
        ],
        name="share",
    )(coded, coded, target, gain)


def grad_kernel(share_ref, stats_ref, target_ref, gain_ref, normed_ref, grad_ref, *copies_refs):
    stats = jnp.sum(stats_ref[...], axis=0)
    features = share_ref.shape[1] * stats_ref.shape[0]
    square, gained, crossed = stats[0:1, :], stats[1:2, :], stats[2:3, :]
    inv_rms = lax.rsqrt(square / features + EPSILON)
    inner = inv_rms * (inv_rms * gained - crossed) / features
    columns = columns_of(jnp.concatenate([inv_rms, inner, jnp.zeros((6, BLOCK), F32)], axis=0))
    inv_col, inner_col = columns[:, 0:1], columns[:, 1:2]
    gain = gain_ref[...]
    normal = share_ref[...] * inv_col
    output = normal * gain
    grad_norm = (output - target_ref[...].astype(F32)) * gain
    grad = (inv_col * (grad_norm - normal * inner_col)).astype(BF16)
    normed_ref[...] = output.astype(BF16)
    grad_ref[...] = grad
    for half, copies_ref in enumerate(copies_refs):
        width = copies_ref.shape[2]
        for part in range(copies_ref.shape[0]):
            copies_ref[part] = grad[:, half * width : (half + 1) * width]


def grads(share, stats, target, gain, pieces):
    tokens, width = share.shape
    parts = stats.shape[0]
    block = pl.BlockSpec((BLOCK, width), lambda i: (i, 0))
    copies = pl.BlockSpec((parts, BLOCK, width // max(pieces, 1)), lambda i: (0, i, 0))
    return pl.pallas_call(
        grad_kernel,
        grid=(tokens // BLOCK,),
        in_specs=[
            block,
            pl.BlockSpec((parts, 8, BLOCK), lambda i: (0, 0, i)),
            block,
            pl.BlockSpec((1, width), lambda i: (0, 0)),
        ],
        out_specs=[block, block] + [copies] * pieces,
        out_shape=[
            jax.ShapeDtypeStruct((tokens, width), BF16),
            jax.ShapeDtypeStruct((tokens, width), BF16),
        ]
        + [jax.ShapeDtypeStruct((parts, tokens, width // pieces), BF16) for _ in range(pieces)],
        name="grads",
    )(share, stats, target, gain)


def updated(rate_ref, hidden_ref, grad, weight):
    weight_grad = jnp.dot(hidden_ref[...], grad, preferred_element_type=F32)
    return (weight.astype(F32) - rate_ref[0] * weight_grad).astype(BF16)


def beside(one, other):
    return jnp.concatenate([one, other], axis=1)


def in_pairs(count, body):
    def both(number, _):
        body(2 * number)
        body(2 * number + 1)
        return 0

    lax.fori_loop(0, count // 2, both, 0)


def update_kernel(rate_ref, hidden_ref, *refs):
    *grad_refs, weight_ref, updated_ref = refs
    parts, _, width = grad_refs[0].shape

    def one_part(part):
        columns = columns_at(part, width * len(grad_refs))
        grad = grad_refs[0][part] if len(grad_refs) == 1 else beside(grad_refs[0][part], grad_refs[1][part])
        updated_ref[:, columns] = updated(rate_ref, hidden_ref, grad, weight_ref[:, columns])

    in_pairs(parts, one_part)


def half_update_kernel(half, rate_ref, hidden_ref, grad_ref, weight_ref, updated_ref):
    parts, _, width = grad_ref.shape

    def one_pair(pair):
        grad = beside(grad_ref[2 * pair], grad_ref[2 * pair + 1])
        weight = beside(*(weight_ref[:, columns_at(4 * pair + 2 * k + half, width)] for k in range(2)))
        updated_ref[:, columns_at(pair, 2 * width)] = updated(rate_ref, hidden_ref, grad, weight)

    in_pairs(parts // 2, one_pair)


def paired_update_kernel(half, rate_ref, hidden_ref, grad_ref, weight_ref, updated_ref):
    pairs, _, width = grad_ref.shape

    def one_pair(pair):
        weight = beside(*(weight_ref[:, columns_at(4 * pair + 2 * k + half, width // 2)] for k in range(2)))
        updated_ref[:, columns_at(pair, width)] = updated(rate_ref, hidden_ref, grad_ref[pair], weight)

    in_pairs(pairs, one_pair)


def update(kernel, rate, hidden_t, grads, weight, first, rows, block, width):
    tokens, features = hidden_t.shape[1], weight.shape[1]
    skip = first // block
    hidden_skip = (hidden_t.shape[0] - weight.shape[0] + first) // block
    return pl.pallas_call(
        kernel,
        grid=(rows // block,),
        in_specs=[
            pl.BlockSpec(memory_space=pltpu.SMEM),
            pl.BlockSpec((block, tokens), lambda i: (i + hidden_skip, 0)),
            *(pl.BlockSpec(memory_space=pltpu.VMEM) for _ in grads),
            pl.BlockSpec((block, features), lambda i: (i + skip, 0)),
        ],
        out_specs=pl.BlockSpec((block, width), lambda i: (i, 0)),
        out_shape=jax.ShapeDtypeStruct((rows, width), BF16),
        name="update",
    )(rate, hidden_t, *grads, weight)


def averaged(one, other):
    return (0.5 * (one.astype(F32) + other.astype(F32))).astype(BF16)


def mix_early_kernel(rate_ref, hidden_ref, grad_ref, weight_ref, own_ref, *refs):
    mixed_ref = refs[-1]
    parts, _, width = grad_ref.shape

    def one_part(part):
        columns = columns_at(part, width)
        peer = updated(rate_ref, hidden_ref, grad_ref[part], weight_ref[:, columns])
        mixed_ref[:, columns] = averaged(own_ref[:, columns], peer)

    in_pairs(parts, one_part)


def mix_early(rate, hidden_t, grad, weight, own, first, block, held, rows):
    early, tokens = hidden_t.shape
    features = weight.shape[1]
    skip = first // block
    kept = () if held is None else (held,)
    here = pl.BlockSpec((block, features), lambda i: (i, 0))
    there = pl.BlockSpec((block, features), lambda i: (i + skip, 0))
    return pl.pallas_call(
        mix_early_kernel,
        grid=(early // block,),
        in_specs=[
            pl.BlockSpec(memory_space=pltpu.SMEM),
            pl.BlockSpec((block, tokens), lambda i: (i, 0)),
            pl.BlockSpec(memory_space=pltpu.VMEM),
            here,
            there,
            *(pl.BlockSpec(memory_space=pl.ANY) for _ in kept),
        ],
        out_specs=there,
        out_shape=jax.ShapeDtypeStruct((rows, features), BF16),
        input_output_aliases={5: 0} if kept else {},
        name="mix_early",
    )(rate, hidden_t, grad, weight, own, *kept)


def mix_late_kernel(own_ref, peer_ref, *refs):
    refs[-1][...] = averaged(own_ref[...], peer_ref[...])


def mix_late(own, peer, piece, pieces, width, first, block, held, rows):
    late, features = own.shape
    kept = () if held is None else (held,)
    skip = first // block
    wide = width // pieces if pieces > 1 else features
    here = pl.BlockSpec((block, wide), lambda i, j: (i, j))
    return pl.pallas_call(
        mix_late_kernel,
        grid=(late // block, features // wide),
        in_specs=[here, here] + [pl.BlockSpec(memory_space=pl.ANY) for _ in kept],
        out_specs=pl.BlockSpec((block, wide), lambda i, j: (i + skip, pieces * j + piece)),
        out_shape=jax.ShapeDtypeStruct((rows, pieces * features), BF16),
        input_output_aliases={2: 0} if kept else {},
        name="mix_late",
    )(own, peer, *kept)


def exchanged(parts, axes=TP):
    return lax.all_to_all(parts, axes, split_axis=0, concat_axis=0, tiled=True)


def step(level, gate, up, target, gain, weight, rate):
    count = lax.axis_size("dp")
    parts = lax.axis_size(TP)
    rows, features = weight.shape
    width = features // parts
    back, straight, block, halves, paired, late_first = PLANS[level]
    early = back + straight
    by = 1 << level

    def sent(array, by):
        return lax.ppermute(array, "dp", [(i, (i + by) % count) for i in range(count)])

    def two_hops(array):
        for _ in range(2):
            array = sent(array, (by - count) // 2)
        return array

    if early:
        peer_weight = sent(weight[back:early], by)
    if back:
        peer_weight_back = two_hops(weight[:back])
    hidden_t, coded = forward(gate, up, weight, parts)
    hidden_late = hidden_t
    if early:
        peer_hidden = sent(hidden_t[back:early], by)
        hidden_late = hidden_t[early - block :]
    if back:
        hidden_back = hidden_t[:back]
        peer_hidden_back = two_hops(hidden_back)
    coded = exchanged(coded)
    share, stats = share_and_stats(coded, target, gain)
    stats = exchanged(stats)
    normed, grad_share, *copies = grads(share, stats, target, gain, 0 if paired else 1 + halves)
    if early:
        peer_share = sent(grad_share, by)
    pieces = 1 + halves
    if paired:
        pairs = lax.axis_size("tp_0")
        other = lax.ppermute(grad_share, "tp_1", [(0, 1), (1, 0)])
        first = lax.axis_index("tp_1") == 0
        piece = width // pieces
        for half in range(pieces):
            one, two = (x[:, half * piece : (half + 1) * piece] for x in (grad_share, other))
            both = jnp.concatenate([jnp.where(first, one, two), jnp.where(first, two, one)], axis=1)
            copies.append(jnp.broadcast_to(both, (pairs, *both.shape)))
    grad = []
    for half in range(pieces):
        grad.append(exchanged(copies[half], "tp_0" if paired else TP))
    rate = rate * FF ** (-0.5)
    own_late, peer_late = [], []
    for half in range(pieces):
        kernel = update_kernel
        if halves:
            kernel = functools.partial(paired_update_kernel if paired else half_update_kernel, half)
        own_late.append(
            update(
                kernel, rate, hidden_late, grad[half : half + 1], weight, early, rows - early, block,
                features // pieces,
            )
        )
        peer_late.append(sent(own_late[half], by))
    mixed = None

    def mix_pieces(mixed):
        tall = math.gcd(early, rows - early) if early else rows
        for piece in range(pieces):
            mixed = mix_late(
                own_late[piece], peer_late[piece], piece, pieces, width, early, tall, mixed, rows
            )
        return mixed

    if early:
        peer_grad = exchanged(jnp.broadcast_to(peer_share, (parts, *peer_share.shape)))
        own_early = update(update_kernel, rate, hidden_t, grad, weight, 0, early, block, features)
    if late_first:
        mixed = mix_pieces(mixed)
    if back:
        mixed = mix_early(
            rate, peer_hidden_back, peer_grad, peer_weight_back, own_early, 0, block, mixed, rows
        )
    if early:
        mixed = mix_early(rate, peer_hidden, peer_grad, peer_weight, own_early, back, block, mixed, rows)
    if not late_first:
        mixed = mix_pieces(mixed)
    return normed, mixed


def shards(gate_pre, up_pre, target, norm_gain, weight, round_index):
    rate = step_rate(round_index).reshape(1)
    levels = lax.axis_size("dp").bit_length() - 1
    level = round_index[0] % levels
    branches = [functools.partial(step, number) for number in range(levels)]
    normed, mixed = lax.switch(level, branches, gate_pre, up_pre, target, norm_gain[None], weight[0], rate)
    return normed, mixed[None]


def solution(mesh):
    finer = Mesh(mesh.devices.reshape(mesh.shape["dp"], 4, 2), ("dp", "tp_0", "tp_1"))
    placed = (P("dp", TP), P("dp", TP), P("dp", TP), P(TP), P("dp", TP, None), P())
    return jax.shard_map(
        shards,
        mesh=finer,
        in_specs=placed,
        out_specs=(P("dp", TP), P("dp", TP, None)),
        check_vma=False,
    )
```

```python
import functools
import math

import jax
import jax.numpy as jnp
from jax import lax
from jax.experimental import pallas as pl
from jax.experimental.pallas import tpu as pltpu
from jax.sharding import Mesh
from jax.sharding import PartitionSpec as P


FF = 7168
EPSILON = 1e-06
TP = ("tp_0", "tp_1")
BLOCK = 128
CODES = 16
F32, BF16 = jnp.float32, jnp.bfloat16

PLANS = (
    (0, 0, 224, True, True, False),
    (0, 0, 224, True, True, False),
    (0, 672, 224, False, False, True),
    (224, 336, 112, False, False, False),
    (0, 384, 128, True, False, False),
)


def step_rate(round_index):
    phase = (round_index[0] % 1000).astype(F32) * jnp.float32(2.0 * math.pi / 1000.0)
    return jnp.float32(0.25) * (jnp.float32(0.55) + jnp.float32(0.45) * jnp.cos(phase))


def columns_of(rows):
    filled = jnp.concatenate([rows, jnp.zeros((BLOCK - rows.shape[0], BLOCK), F32)], axis=0)
    return filled.T


def columns_at(number, width):
    return pl.ds(pl.multiple_of(number * width, width), width)


def forward_kernel(gate_ref, up_ref, weight_ref, hidden_t_ref, coded_ref, scale_scr, partial_scr):
    step = pl.program_id(0)
    hidden = jax.nn.silu(gate_ref[...].astype(F32)) * up_ref[...].astype(F32)
    hidden_t_ref[...] = hidden.T.astype(BF16)
    hidden = hidden.astype(BF16)
    parts, _, width = coded_ref.shape

    partial = jnp.dot(hidden, weight_ref[...], preferred_element_type=F32) * FF ** (-0.5)
    top = jnp.max(jnp.abs(partial), axis=1, keepdims=True)
    for part in range(parts):
        partial_scr[part] = partial[:, part * width : (part + 1) * width]
    level = jnp.ceil(8.0 * jnp.log2(jnp.maximum(top, 1e-30))) + 1.0
    factor = jnp.exp2(15.0 - 0.125 * level)
    rows = pl.ds(pl.multiple_of(step * BLOCK, BLOCK), BLOCK)

    def coding(part, _):
        coded_ref[part, rows, :] = jnp.round(partial_scr[part] * factor).astype(jnp.int32).astype(jnp.int16)
        return 0

    lax.fori_loop(0, parts, coding, 0)
    scale_scr[pl.ds(step, 1), :] = jnp.broadcast_to(level, (BLOCK, BLOCK)).T[:1, :]

    @pl.when(step == pl.num_programs(0) - 1)
    def _():
        codes = scale_scr[...].astype(jnp.int32).astype(jnp.int16)
        tokens = coded_ref.shape[1] - CODES
        for part in range(parts):
            coded_ref[part, tokens:, :BLOCK] = codes
            coded_ref[part, tokens:, BLOCK:] = codes


def forward(gate, up, weight, parts):
    tokens, units = gate.shape
    width = weight.shape[1] // parts
    return pl.pallas_call(
        forward_kernel,
        grid=(tokens // BLOCK,),
        in_specs=[
            pl.BlockSpec((BLOCK, units), lambda i: (i, 0)),
            pl.BlockSpec((BLOCK, units), lambda i: (i, 0)),
            pl.BlockSpec(weight.shape, lambda i: (0, 0)),
        ],
        out_specs=[
            pl.BlockSpec((units, BLOCK), lambda i: (0, i)),
            pl.BlockSpec((parts, tokens + CODES, width), lambda i: (0, 0, 0)),
        ],
        out_shape=[
            jax.ShapeDtypeStruct((units, tokens), BF16),
            jax.ShapeDtypeStruct((parts, tokens + CODES, width), jnp.int16),
        ],
        scratch_shapes=[pltpu.VMEM((CODES, BLOCK), F32), pltpu.VMEM((parts, BLOCK, width), F32)],
        name="forward",
    )(gate, up, weight)


def share_kernel(coded_ref, codes_ref, target_ref, gain_ref, share_ref, stats_ref):
    step = pl.program_id(0)
    parts = coded_ref.shape[0]
    codes = codes_ref[...][:, :, :BLOCK].astype(jnp.int32).astype(F32)
    here = lax.broadcasted_iota(jnp.int32, codes.shape, 1) == step
    factors = columns_of(jnp.exp2(0.125 * jnp.sum(jnp.where(here, codes, 0.0), axis=1) - 15.0))
    share = jnp.zeros(share_ref.shape, F32)
    for part in range(parts):
        share += coded_ref[part].astype(jnp.int32).astype(F32) * factors[:, part : part + 1]
    share_ref[...] = share
    gain = gain_ref[...]
    scaled = share * gain
    square = jnp.sum(share * share, axis=1, keepdims=True)
    gained = jnp.sum(scaled * scaled, axis=1, keepdims=True)
    crossed = jnp.sum(target_ref[...].astype(F32) * scaled, axis=1, keepdims=True)
    lane = lax.broadcasted_iota(jnp.int32, (BLOCK, BLOCK), 1)
    packed = jnp.where(lane == 0, square, jnp.where(lane == 1, gained, jnp.where(lane == 2, crossed, 0.0)))
    stats = packed.T[:8, :]
    for part in range(parts):
        stats_ref[part] = stats


def share_and_stats(coded, target, gain):
    parts, _, width = coded.shape
    tokens = target.shape[0]
    return pl.pallas_call(
        share_kernel,
        grid=(tokens // BLOCK,),
        in_specs=[
            pl.BlockSpec((parts, BLOCK, width), lambda i: (0, i, 0)),
            pl.BlockSpec((parts, CODES, width), lambda i: (0, tokens // CODES, 0)),
            pl.BlockSpec((BLOCK, width), lambda i: (i, 0)),
            pl.BlockSpec((1, width), lambda i: (0, 0)),
        ],
        out_specs=[
            pl.BlockSpec((BLOCK, width), lambda i: (i, 0)),
            pl.BlockSpec((parts, 8, BLOCK), lambda i: (0, 0, i)),
        ],
        out_shape=[
            jax.ShapeDtypeStruct((tokens, width), F32),
            jax.ShapeDtypeStruct((parts, 8, tokens), F32),
        ],
        name="share",
    )(coded, coded, target, gain)


def grad_kernel(share_ref, stats_ref, target_ref, gain_ref, normed_ref, grad_ref, *copies_refs):
    stats = jnp.sum(stats_ref[...], axis=0)
    features = share_ref.shape[1] * stats_ref.shape[0]
    square, gained, crossed = stats[0:1, :], stats[1:2, :], stats[2:3, :]
    inv_rms = lax.rsqrt(square / features + EPSILON)
    inner = inv_rms * (inv_rms * gained - crossed) / features
    columns = columns_of(jnp.concatenate([inv_rms, inner, jnp.zeros((6, BLOCK), F32)], axis=0))
    inv_col, inner_col = columns[:, 0:1], columns[:, 1:2]
    gain = gain_ref[...]
    normal = share_ref[...] * inv_col
    output = normal * gain
    grad_norm = (output - target_ref[...].astype(F32)) * gain
    grad = (inv_col * (grad_norm - normal * inner_col)).astype(BF16)
    normed_ref[...] = output.astype(BF16)
    grad_ref[...] = grad
    for half, copies_ref in enumerate(copies_refs):
        width = copies_ref.shape[2]
        for part in range(copies_ref.shape[0]):
            copies_ref[part] = grad[:, half * width : (half + 1) * width]


def grads(share, stats, target, gain, pieces):
    tokens, width = share.shape
    parts = stats.shape[0]
    block = pl.BlockSpec((BLOCK, width), lambda i: (i, 0))
    copies = pl.BlockSpec((parts, BLOCK, width // max(pieces, 1)), lambda i: (0, i, 0))
    return pl.pallas_call(
        grad_kernel,
        grid=(tokens // BLOCK,),
        in_specs=[
            block,
            pl.BlockSpec((parts, 8, BLOCK), lambda i: (0, 0, i)),
            block,
            pl.BlockSpec((1, width), lambda i: (0, 0)),
        ],
        out_specs=[block, block] + [copies] * pieces,
        out_shape=[
            jax.ShapeDtypeStruct((tokens, width), BF16),
            jax.ShapeDtypeStruct((tokens, width), BF16),
        ]
        + [jax.ShapeDtypeStruct((parts, tokens, width // pieces), BF16) for _ in range(pieces)],
        name="grads",
    )(share, stats, target, gain)


def updated(rate_ref, hidden_ref, grad, weight):
    weight_grad = jnp.dot(hidden_ref[...], grad, preferred_element_type=F32)
    return (weight.astype(F32) - rate_ref[0] * weight_grad).astype(BF16)


def beside(one, other):
    return jnp.concatenate([one, other], axis=1)


def in_pairs(count, body):
    def both(number, _):
        body(2 * number)
        body(2 * number + 1)
        return 0

    lax.fori_loop(0, count // 2, both, 0)


def update_kernel(rate_ref, hidden_ref, *refs):
    *grad_refs, weight_ref, updated_ref = refs
    parts, _, width = grad_refs[0].shape

    def one_part(part):
        columns = columns_at(part, width * len(grad_refs))
        grad = grad_refs[0][part] if len(grad_refs) == 1 else beside(grad_refs[0][part], grad_refs[1][part])
        updated_ref[:, columns] = updated(rate_ref, hidden_ref, grad, weight_ref[:, columns])

    in_pairs(parts, one_part)


def half_update_kernel(half, rate_ref, hidden_ref, grad_ref, weight_ref, updated_ref):
    parts, _, width = grad_ref.shape

    def one_pair(pair):
        grad = beside(grad_ref[2 * pair], grad_ref[2 * pair + 1])
        weight = beside(*(weight_ref[:, columns_at(4 * pair + 2 * k + half, width)] for k in range(2)))
        updated_ref[:, columns_at(pair, 2 * width)] = updated(rate_ref, hidden_ref, grad, weight)

    in_pairs(parts // 2, one_pair)


def paired_update_kernel(half, rate_ref, hidden_ref, grad_ref, weight_ref, updated_ref):
    pairs, _, width = grad_ref.shape

    def one_pair(pair):
        weight = beside(*(weight_ref[:, columns_at(4 * pair + 2 * k + half, width // 2)] for k in range(2)))
        updated_ref[:, columns_at(pair, width)] = updated(rate_ref, hidden_ref, grad_ref[pair], weight)

    in_pairs(pairs, one_pair)


def update(kernel, rate, hidden_t, grads, weight, first, rows, block, width):
    tokens, features = hidden_t.shape[1], weight.shape[1]
    skip = first // block
    hidden_skip = (hidden_t.shape[0] - weight.shape[0] + first) // block
    return pl.pallas_call(
        kernel,
        grid=(rows // block,),
        in_specs=[
            pl.BlockSpec(memory_space=pltpu.SMEM),
            pl.BlockSpec((block, tokens), lambda i: (i + hidden_skip, 0)),
            *(pl.BlockSpec(memory_space=pltpu.VMEM) for _ in grads),
            pl.BlockSpec((block, features), lambda i: (i + skip, 0)),
        ],
        out_specs=pl.BlockSpec((block, width), lambda i: (i, 0)),
        out_shape=jax.ShapeDtypeStruct((rows, width), BF16),
        name="update",
    )(rate, hidden_t, *grads, weight)


def averaged(one, other):
    return (0.5 * (one.astype(F32) + other.astype(F32))).astype(BF16)


def mix_early_kernel(rate_ref, hidden_ref, grad_ref, weight_ref, own_ref, *refs):
    mixed_ref = refs[-1]
    parts, _, width = grad_ref.shape

    def one_part(part):
        columns = columns_at(part, width)
        peer = updated(rate_ref, hidden_ref, grad_ref[part], weight_ref[:, columns])
        mixed_ref[:, columns] = averaged(own_ref[:, columns], peer)

    in_pairs(parts, one_part)


def mix_early(rate, hidden_t, grad, weight, own, first, block, held, rows):
    early, tokens = hidden_t.shape
    features = weight.shape[1]
    skip = first // block
    kept = () if held is None else (held,)
    here = pl.BlockSpec((block, features), lambda i: (i, 0))
    there = pl.BlockSpec((block, features), lambda i: (i + skip, 0))
    return pl.pallas_call(
        mix_early_kernel,
        grid=(early // block,),
        in_specs=[
            pl.BlockSpec(memory_space=pltpu.SMEM),
            pl.BlockSpec((block, tokens), lambda i: (i, 0)),
            pl.BlockSpec(memory_space=pltpu.VMEM),
            here,
            there,
            *(pl.BlockSpec(memory_space=pl.ANY) for _ in kept),
        ],
        out_specs=there,
        out_shape=jax.ShapeDtypeStruct((rows, features), BF16),
        input_output_aliases={5: 0} if kept else {},
        name="mix_early",
    )(rate, hidden_t, grad, weight, own, *kept)


def mix_late_kernel(pieces, width, *refs):
    own_refs, peer_refs, mixed_ref = refs[:pieces], refs[pieces : 2 * pieces], refs[-1]

    def one_part(part, _):
        columns = columns_at(part, width)
        for piece in range(pieces):
            mixed_ref[:, columns_at(part * pieces + piece, width)] = averaged(
                own_refs[piece][:, columns], peer_refs[piece][:, columns]
            )
        return 0

    lax.fori_loop(0, own_refs[0].shape[1] // width, one_part, 0)


def mix_late(own, peer, width, first, block, held, rows):
    late, features = own[0].shape
    pieces = len(own)
    kept = () if held is None else (held,)
    skip = first // block
    here = pl.BlockSpec((block, features), lambda i: (i, 0))
    return pl.pallas_call(
        functools.partial(mix_late_kernel, pieces, width // pieces),
        grid=(late // block,),
        in_specs=[here] * (2 * pieces) + [pl.BlockSpec(memory_space=pl.ANY) for _ in kept],
        out_specs=pl.BlockSpec((block, pieces * features), lambda i: (i + skip, 0)),
        out_shape=jax.ShapeDtypeStruct((rows, pieces * features), BF16),
        input_output_aliases={2 * pieces: 0} if kept else {},
        name="mix_late",
    )(*own, *peer, *kept)


def exchanged(parts, axes=TP):
    return lax.all_to_all(parts, axes, split_axis=0, concat_axis=0, tiled=True)


def step(level, gate, up, target, gain, weight, rate):
    count = lax.axis_size("dp")
    parts = lax.axis_size(TP)
    rows, features = weight.shape
    width = features // parts
    back, straight, block, halves, paired, late_first = PLANS[level]
    early = back + straight
    by = 1 << level

    def sent(array, by):
        return lax.ppermute(array, "dp", [(i, (i + by) % count) for i in range(count)])

    def two_hops(array):
        for _ in range(2):
            array = sent(array, (by - count) // 2)
        return array

    if early:
        peer_weight = sent(weight[back:early], by)
    if back:
        weight_back = weight[:back]
        peer_weight_back = two_hops(weight_back)
    hidden_t, coded = forward(gate, up, weight, parts)
    hidden_late = hidden_t
    if early:
        peer_hidden = sent(hidden_t[back:early], by)
        hidden_late = hidden_t[early - block :]
    if back:
        hidden_back = hidden_t[:back]
        peer_hidden_back = two_hops(hidden_back)
    coded = exchanged(coded)
    share, stats = share_and_stats(coded, target, gain)
    stats = exchanged(stats)
    normed, grad_share, *copies = grads(share, stats, target, gain, 0 if paired else 1 + halves)
    if early:
        peer_share = sent(grad_share, by)
    pieces = 1 + halves
    if paired:
        pairs = lax.axis_size("tp_0")
        other = lax.ppermute(grad_share, "tp_1", [(0, 1), (1, 0)])
        first = lax.axis_index("tp_1") == 0
        piece = width // pieces
        for half in range(pieces):
            one, two = (x[:, half * piece : (half + 1) * piece] for x in (grad_share, other))
            both = jnp.concatenate([jnp.where(first, one, two), jnp.where(first, two, one)], axis=1)
            copies.append(jnp.broadcast_to(both, (pairs, *both.shape)))
    grad = []
    for half in range(pieces):
        grad.append(exchanged(copies[half], "tp_0" if paired else TP))
    rate = rate * FF ** (-0.5)
    own_late, peer_late = [], []
    for half in range(pieces):
        kernel = update_kernel
        if halves:
            kernel = functools.partial(paired_update_kernel if paired else half_update_kernel, half)
        own_late.append(
            update(
                kernel, rate, hidden_late, grad[half : half + 1], weight, early, rows - early, block,
                features // pieces,
            )
        )
        peer_late.append(sent(own_late[half], by))
    mixed = None

    def mix_pieces(mixed):
        return mix_late(own_late, peer_late, width, early, block, mixed, rows)

    if early:
        peer_grad = exchanged(jnp.broadcast_to(peer_share, (parts, *peer_share.shape)))
        own_early = update(update_kernel, rate, hidden_t, grad, weight, 0, early, block, features)
    if late_first:
        mixed = mix_pieces(mixed)
    if early:
        mixed = mix_early(rate, peer_hidden, peer_grad, peer_weight, own_early, back, block, mixed, rows)
    if back:
        mixed = mix_early(
            rate, peer_hidden_back, peer_grad, peer_weight_back, own_early, 0, block, mixed, rows
        )
    if not late_first:
        mixed = mix_pieces(mixed)
    return normed, mixed


def shards(gate_pre, up_pre, target, norm_gain, weight, round_index):
    rate = step_rate(round_index).reshape(1)
    levels = lax.axis_size("dp").bit_length() - 1
    level = round_index[0] % levels
    branches = [functools.partial(step, number) for number in range(levels)]
    normed, mixed = lax.switch(level, branches, gate_pre, up_pre, target, norm_gain[None], weight[0], rate)
    return normed, mixed[None]


def solution(mesh):
    finer = Mesh(mesh.devices.reshape(mesh.shape["dp"], 4, 2), ("dp", "tp_0", "tp_1"))
    placed = (P("dp", TP), P("dp", TP), P("dp", TP), P(TP), P("dp", TP, None), P())
    return jax.shard_map(
        shards,
        mesh=finer,
        in_specs=placed,
        out_specs=(P("dp", TP), P("dp", TP, None)),
        check_vma=False,
    )
```

```python
import functools
import math

import jax
import jax.numpy as jnp
from jax import lax
from jax.experimental import pallas as pl
from jax.experimental.pallas import tpu as pltpu
from jax.sharding import Mesh
from jax.sharding import PartitionSpec as P


FF = 7168
EPSILON = 1e-06
TP = ("tp_0", "tp_1")
BLOCK = 128
CODES = 16
F32, BF16 = jnp.float32, jnp.bfloat16

PLANS = (
    (0, 0, 224, True, True, False),
    (0, 0, 224, True, True, False),
    (0, 560, 112, False, False, False),
    (224, 336, 112, False, False, False),
    (0, 384, 128, True, False, False),
)


def step_rate(round_index):
    phase = (round_index[0] % 1000).astype(F32) * jnp.float32(2.0 * math.pi / 1000.0)
    return jnp.float32(0.25) * (jnp.float32(0.55) + jnp.float32(0.45) * jnp.cos(phase))


def columns_of(rows):
    filled = jnp.concatenate([rows, jnp.zeros((BLOCK - rows.shape[0], BLOCK), F32)], axis=0)
    return filled.T


def columns_at(number, width):
    return pl.ds(pl.multiple_of(number * width, width), width)


def forward_kernel(gate_ref, up_ref, weight_ref, hidden_t_ref, coded_ref, scale_scr, partial_scr):
    step = pl.program_id(0)
    hidden = jax.nn.silu(gate_ref[...].astype(F32)) * up_ref[...].astype(F32)
    hidden_t_ref[...] = hidden.T.astype(BF16)
    hidden = hidden.astype(BF16)
    parts, _, width = coded_ref.shape

    partial = jnp.dot(hidden, weight_ref[...], preferred_element_type=F32) * FF ** (-0.5)
    top = jnp.max(jnp.abs(partial), axis=1, keepdims=True)
    for part in range(parts):
        partial_scr[part] = partial[:, part * width : (part + 1) * width]
    level = jnp.ceil(8.0 * jnp.log2(jnp.maximum(top, 1e-30))) + 1.0
    factor = jnp.exp2(15.0 - 0.125 * level)
    rows = pl.ds(pl.multiple_of(step * BLOCK, BLOCK), BLOCK)

    def coding(part, _):
        coded_ref[part, rows, :] = jnp.round(partial_scr[part] * factor).astype(jnp.int32).astype(jnp.int16)
        return 0

    lax.fori_loop(0, parts, coding, 0)
    scale_scr[pl.ds(step, 1), :] = jnp.broadcast_to(level, (BLOCK, BLOCK)).T[:1, :]

    @pl.when(step == pl.num_programs(0) - 1)
    def _():
        codes = scale_scr[...].astype(jnp.int32).astype(jnp.int16)
        tokens = coded_ref.shape[1] - CODES
        for part in range(parts):
            coded_ref[part, tokens:, :BLOCK] = codes
            coded_ref[part, tokens:, BLOCK:] = codes


def forward(gate, up, weight, parts):
    tokens, units = gate.shape
    width = weight.shape[1] // parts
    return pl.pallas_call(
        forward_kernel,
        grid=(tokens // BLOCK,),
        in_specs=[
            pl.BlockSpec((BLOCK, units), lambda i: (i, 0)),
            pl.BlockSpec((BLOCK, units), lambda i: (i, 0)),
            pl.BlockSpec(weight.shape, lambda i: (0, 0)),
        ],
        out_specs=[
            pl.BlockSpec((units, BLOCK), lambda i: (0, i)),
            pl.BlockSpec((parts, tokens + CODES, width), lambda i: (0, 0, 0)),
        ],
        out_shape=[
            jax.ShapeDtypeStruct((units, tokens), BF16),
            jax.ShapeDtypeStruct((parts, tokens + CODES, width), jnp.int16),
        ],
        scratch_shapes=[pltpu.VMEM((CODES, BLOCK), F32), pltpu.VMEM((parts, BLOCK, width), F32)],
        name="forward",
    )(gate, up, weight)


def share_kernel(coded_ref, codes_ref, target_ref, gain_ref, share_ref, stats_ref):
    step = pl.program_id(0)
    parts = coded_ref.shape[0]
    codes = codes_ref[...][:, :, :BLOCK].astype(jnp.int32).astype(F32)
    here = lax.broadcasted_iota(jnp.int32, codes.shape, 1) == step
    factors = columns_of(jnp.exp2(0.125 * jnp.sum(jnp.where(here, codes, 0.0), axis=1) - 15.0))
    share = jnp.zeros(share_ref.shape, F32)
    for part in range(parts):
        share += coded_ref[part].astype(jnp.int32).astype(F32) * factors[:, part : part + 1]
    share_ref[...] = share
    gain = gain_ref[...]
    scaled = share * gain
    square = jnp.sum(share * share, axis=1, keepdims=True)
    gained = jnp.sum(scaled * scaled, axis=1, keepdims=True)
    crossed = jnp.sum(target_ref[...].astype(F32) * scaled, axis=1, keepdims=True)
    lane = lax.broadcasted_iota(jnp.int32, (BLOCK, BLOCK), 1)
    packed = jnp.where(lane == 0, square, jnp.where(lane == 1, gained, jnp.where(lane == 2, crossed, 0.0)))
    stats = packed.T[:8, :]
    for part in range(parts):
        stats_ref[part] = stats


def share_and_stats(coded, target, gain):
    parts, _, width = coded.shape
    tokens = target.shape[0]
    return pl.pallas_call(
        share_kernel,
        grid=(tokens // BLOCK,),
        in_specs=[
            pl.BlockSpec((parts, BLOCK, width), lambda i: (0, i, 0)),
            pl.BlockSpec((parts, CODES, width), lambda i: (0, tokens // CODES, 0)),
            pl.BlockSpec((BLOCK, width), lambda i: (i, 0)),
            pl.BlockSpec((1, width), lambda i: (0, 0)),
        ],
        out_specs=[
            pl.BlockSpec((BLOCK, width), lambda i: (i, 0)),
            pl.BlockSpec((parts, 8, BLOCK), lambda i: (0, 0, i)),
        ],
        out_shape=[
            jax.ShapeDtypeStruct((tokens, width), F32),
            jax.ShapeDtypeStruct((parts, 8, tokens), F32),
        ],
        name="share",
    )(coded, coded, target, gain)


def grad_kernel(share_ref, stats_ref, target_ref, gain_ref, normed_ref, grad_ref, *copies_refs):
    stats = jnp.sum(stats_ref[...], axis=0)
    features = share_ref.shape[1] * stats_ref.shape[0]
    square, gained, crossed = stats[0:1, :], stats[1:2, :], stats[2:3, :]
    inv_rms = lax.rsqrt(square / features + EPSILON)
    inner = inv_rms * (inv_rms * gained - crossed) / features
    columns = columns_of(jnp.concatenate([inv_rms, inner, jnp.zeros((6, BLOCK), F32)], axis=0))
    inv_col, inner_col = columns[:, 0:1], columns[:, 1:2]
    gain = gain_ref[...]
    normal = share_ref[...] * inv_col
    output = normal * gain
    grad_norm = (output - target_ref[...].astype(F32)) * gain
    grad = (inv_col * (grad_norm - normal * inner_col)).astype(BF16)
    normed_ref[...] = output.astype(BF16)
    grad_ref[...] = grad
    for half, copies_ref in enumerate(copies_refs):
        width = copies_ref.shape[2]
        for part in range(copies_ref.shape[0]):
            copies_ref[part] = grad[:, half * width : (half + 1) * width]


def grads(share, stats, target, gain, pieces):
    tokens, width = share.shape
    parts = stats.shape[0]
    block = pl.BlockSpec((BLOCK, width), lambda i: (i, 0))
    copies = pl.BlockSpec((parts, BLOCK, width // max(pieces, 1)), lambda i: (0, i, 0))
    return pl.pallas_call(
        grad_kernel,
        grid=(tokens // BLOCK,),
        in_specs=[
            block,
            pl.BlockSpec((parts, 8, BLOCK), lambda i: (0, 0, i)),
            block,
            pl.BlockSpec((1, width), lambda i: (0, 0)),
        ],
        out_specs=[block, block] + [copies] * pieces,
        out_shape=[
            jax.ShapeDtypeStruct((tokens, width), BF16),
            jax.ShapeDtypeStruct((tokens, width), BF16),
        ]
        + [jax.ShapeDtypeStruct((parts, tokens, width // pieces), BF16) for _ in range(pieces)],
        name="grads",
    )(share, stats, target, gain)


def updated(rate_ref, hidden_ref, grad, weight):
    weight_grad = jnp.dot(hidden_ref[...], grad, preferred_element_type=F32)
    return (weight.astype(F32) - rate_ref[0] * weight_grad).astype(BF16)


def beside(one, other):
    return jnp.concatenate([one, other], axis=1)


def in_fours(count, body):
    def four(number, _):
        for k in range(4):
            body(4 * number + k)
        return 0

    lax.fori_loop(0, count // 4, four, 0)


def update_kernel(rate_ref, hidden_ref, *refs):
    *grad_refs, weight_ref, updated_ref = refs
    parts, _, width = grad_refs[0].shape

    def one_part(part):
        columns = columns_at(part, width * len(grad_refs))
        grad = grad_refs[0][part] if len(grad_refs) == 1 else beside(grad_refs[0][part], grad_refs[1][part])
        updated_ref[:, columns] = updated(rate_ref, hidden_ref, grad, weight_ref[:, columns])

    in_fours(parts, one_part)


def half_update_kernel(half, rate_ref, hidden_ref, grad_ref, weight_ref, updated_ref):
    parts, _, width = grad_ref.shape

    def one_pair(pair):
        grad = beside(grad_ref[2 * pair], grad_ref[2 * pair + 1])
        weight = beside(*(weight_ref[:, columns_at(4 * pair + 2 * k + half, width)] for k in range(2)))
        updated_ref[:, columns_at(pair, 2 * width)] = updated(rate_ref, hidden_ref, grad, weight)

    in_fours(parts // 2, one_pair)


def paired_update_kernel(half, rate_ref, hidden_ref, grad_ref, weight_ref, updated_ref):
    pairs, _, width = grad_ref.shape

    def one_pair(pair):
        weight = beside(*(weight_ref[:, columns_at(4 * pair + 2 * k + half, width // 2)] for k in range(2)))
        updated_ref[:, columns_at(pair, width)] = updated(rate_ref, hidden_ref, grad_ref[pair], weight)

    in_fours(pairs, one_pair)


def update(kernel, rate, hidden_t, grads, weight, first, rows, block, width):
    tokens, features = hidden_t.shape[1], weight.shape[1]
    skip = first // block
    hidden_skip = (hidden_t.shape[0] - weight.shape[0] + first) // block
    return pl.pallas_call(
        kernel,
        grid=(rows // block,),
        in_specs=[
            pl.BlockSpec(memory_space=pltpu.SMEM),
            pl.BlockSpec((block, tokens), lambda i: (i + hidden_skip, 0)),
            *(pl.BlockSpec(memory_space=pltpu.VMEM) for _ in grads),
            pl.BlockSpec((block, features), lambda i: (i + skip, 0)),
        ],
        out_specs=pl.BlockSpec((block, width), lambda i: (i, 0)),
        out_shape=jax.ShapeDtypeStruct((rows, width), BF16),
        name="update",
    )(rate, hidden_t, *grads, weight)


def averaged(one, other):
    return (0.5 * (one.astype(F32) + other.astype(F32))).astype(BF16)


def mix_early_kernel(rate_ref, hidden_ref, grad_ref, weight_ref, own_ref, *refs):
    mixed_ref = refs[-1]
    parts, _, width = grad_ref.shape

    def one_part(part):
        columns = columns_at(part, width)
        peer = updated(rate_ref, hidden_ref, grad_ref[part], weight_ref[:, columns])
        mixed_ref[:, columns] = averaged(own_ref[:, columns], peer)

    in_fours(parts, one_part)


def mix_early(rate, hidden_t, grad, weight, own, first, block, held, rows):
    early, tokens = hidden_t.shape
    features = weight.shape[1]
    skip = first // block
    kept = () if held is None else (held,)
    here = pl.BlockSpec((block, features), lambda i: (i, 0))
    there = pl.BlockSpec((block, features), lambda i: (i + skip, 0))
    return pl.pallas_call(
        mix_early_kernel,
        grid=(early // block,),
        in_specs=[
            pl.BlockSpec(memory_space=pltpu.SMEM),
            pl.BlockSpec((block, tokens), lambda i: (i, 0)),
            pl.BlockSpec(memory_space=pltpu.VMEM),
            here,
            there,
            *(pl.BlockSpec(memory_space=pl.ANY) for _ in kept),
        ],
        out_specs=there,
        out_shape=jax.ShapeDtypeStruct((rows, features), BF16),
        input_output_aliases={5: 0} if kept else {},
        name="mix_early",
    )(rate, hidden_t, grad, weight, own, *kept)


def mix_late_kernel(pieces, width, *refs):
    own_refs, peer_refs, mixed_ref = refs[:pieces], refs[pieces : 2 * pieces], refs[-1]

    def one_part(part, _):
        columns = columns_at(part, width)
        for piece in range(pieces):
            mixed_ref[:, columns_at(part * pieces + piece, width)] = averaged(
                own_refs[piece][:, columns], peer_refs[piece][:, columns]
            )
        return 0

    lax.fori_loop(0, own_refs[0].shape[1] // width, one_part, 0)


def mix_late(own, peer, width, first, block, held, rows):
    late, features = own[0].shape
    pieces = len(own)
    kept = () if held is None else (held,)
    skip = first // block
    here = pl.BlockSpec((block, features), lambda i: (i, 0))
    return pl.pallas_call(
        functools.partial(mix_late_kernel, pieces, width // pieces),
        grid=(late // block,),
        in_specs=[here] * (2 * pieces) + [pl.BlockSpec(memory_space=pl.ANY) for _ in kept],
        out_specs=pl.BlockSpec((block, pieces * features), lambda i: (i + skip, 0)),
        out_shape=jax.ShapeDtypeStruct((rows, pieces * features), BF16),
        input_output_aliases={2 * pieces: 0} if kept else {},
        name="mix_late",
    )(*own, *peer, *kept)


def exchanged(parts, axes=TP):
    return lax.all_to_all(parts, axes, split_axis=0, concat_axis=0, tiled=True)


SWAP = [(0, 1), (1, 0)]


def step(level, prepared, gate, up, target, gain, weight, rate):
    count = lax.axis_size("dp")
    parts = lax.axis_size(TP)
    rows, features = weight.shape
    width = features // parts
    back, straight, block, halves, paired, late_first = PLANS[level]
    early = back + straight
    by = 1 << level

    def sent(array, by):
        return lax.ppermute(array, "dp", [(i, (i + by) % count) for i in range(count)])

    def two_hops(array):
        for _ in range(2):
            array = sent(array, (by - count) // 2)
        return array

    if early:
        peer_weight = sent(weight[back:early], by)
    if back:
        weight_back = weight[:back]
        peer_weight_back = two_hops(weight_back)
    hidden_t, coded = prepared or forward(gate, up, weight, parts)
    hidden_late = hidden_t
    if early:
        peer_hidden = sent(hidden_t[back:early], by)
        hidden_late = hidden_t[early - block :]
    if back:
        hidden_back = hidden_t[:back]
        peer_hidden_back = two_hops(hidden_back)
    coded = exchanged(coded)
    share, stats = share_and_stats(coded, target, gain)
    stats = exchanged(stats)
    normed, grad_share, *copies = grads(share, stats, target, gain, 0 if paired else 1 + halves)
    if early:
        peer_share = sent(grad_share, by)
    pieces = 1 + halves
    pairs = lax.axis_size("tp_0")

    def with_other(own, other):
        first = lax.axis_index("tp_1") == 0
        both = jnp.concatenate([jnp.where(first, own, other), jnp.where(first, other, own)], axis=1)
        return jnp.broadcast_to(both, (pairs, *both.shape))

    if paired:
        other = lax.ppermute(grad_share, "tp_1", SWAP)
        piece = width // pieces
        for half in range(pieces):
            copies.append(with_other(*(x[:, half * piece : (half + 1) * piece] for x in (grad_share, other))))
    grad = []
    for half in range(pieces):
        grad.append(exchanged(copies[half], "tp_0" if paired else TP))
    rate = rate * FF ** (-0.5)
    own_late, peer_late = [], []
    for half in range(pieces):
        kernel = update_kernel
        if halves:
            kernel = functools.partial(paired_update_kernel if paired else half_update_kernel, half)
        own_late.append(
            update(
                kernel, rate, hidden_late, grad[half : half + 1], weight, early, rows - early, block,
                features // pieces,
            )
        )
        peer_late.append(sent(own_late[half], by))
    mixed = None

    def mix_pieces(mixed):
        return mix_late(own_late, peer_late, width, early, block, mixed, rows)

    if early:
        peer_grad = exchanged(jnp.broadcast_to(peer_share, (parts, *peer_share.shape)))
        own_early = update(update_kernel, rate, hidden_t, grad, weight, 0, early, block, features)
    if late_first:
        mixed = mix_pieces(mixed)
    if early:
        mixed = mix_early(rate, peer_hidden, peer_grad, peer_weight, own_early, back, block, mixed, rows)
    if back:
        mixed = mix_early(
            rate, peer_hidden_back, peer_grad, peer_weight_back, own_early, 0, block, mixed, rows
        )
    if not late_first:
        mixed = mix_pieces(mixed)
    return normed, mixed


def shards(gate_pre, up_pre, target, norm_gain, weight, round_index):
    rate = step_rate(round_index).reshape(1)
    levels = lax.axis_size("dp").bit_length() - 1
    level = round_index[0] % levels
    operands = (gate_pre, up_pre, target, norm_gain[None], weight[0], rate)
    last = levels - 1

    def forward_first(*operands):
        prepared = forward(operands[0], operands[1], operands[4], lax.axis_size(TP))
        branches = [
            lambda prepared, operands, number=number: step(number, prepared, *operands) for number in range(last)
        ]
        return lax.switch(level, branches, prepared, operands)

    normed, mixed = lax.cond(level == last, functools.partial(step, last, None), forward_first, *operands)
    return normed, mixed[None]


def solution(mesh):
    finer = Mesh(mesh.devices.reshape(mesh.shape["dp"], 4, 2), ("dp", "tp_0", "tp_1"))
    placed = (P("dp", TP), P("dp", TP), P("dp", TP), P(TP), P("dp", TP, None), P())
    return jax.shard_map(
        shards,
        mesh=finer,
        in_specs=placed,
        out_specs=(P("dp", TP), P("dp", TP, None)),
        check_vma=False,
    )
```
